256 devices in a mesh: rep: 2 (over y), tp: 32 (over z, core), sub: 4 (over x).
Axes of the slice: x: 4, y: 2, z: 16, core: 2. Of those that a mesh axis runs over, the one named last changes fastest.
The devices are a block of a 4x16x16 slice.
Arguments:
- hidden_in: bfloat16 [128, 6144], P(('rep', 'sub'), 'tp'), parts along dimension 0, may hold values from -128 to 128
- query: bfloat16 [128, 6144], P(('rep', 'sub'), 'tp'), parts along dimension 0, may hold values from -128 to 128
- key_new: bfloat16 [128, 1024], P(('rep', 'sub'), 'tp'), parts along dimension 0, may hold values from -8 to 8
- value_new: bfloat16 [128, 1024], P(('rep', 'sub'), 'tp'), parts along dimension 0, may hold values from -6 to 6
- key_cache: bfloat16 [128, 1024, 1024], P(('rep', 'sub'), 'tp'), parts along dimension 0, may hold values from -8 to 8
- value_cache: bfloat16 [128, 1024, 1024], P(('rep', 'sub'), 'tp'), parts along dimension 0, may hold values from -6 to 6
- lengths: int32 [128], P(('rep', 'sub')), parts along dimension 0, may hold values from 2 to 1024
- out_weight: bfloat16 [6144, 6144], P('sub', 'tp'), may hold values from -0.078125 to 0.078125
- norm_gain: bfloat16 [6144], P('tp'), may hold values from 0.099609375 to 1.8984375
- router_weight: bfloat16 [6144, 4], P('tp'), may hold values from -0.078125 to 0.078125
- routes: int32 [128, 2], P(('rep', 'sub')), parts along dimension 0, may hold values from 0 to 3, all different within a row; in each aligned block of 16 rows (0 to 15, 16 to 31, ...) at most 12 rows name the same one
- gate_weight: bfloat16 [4, 6144, 8192], P('sub', None, 'tp'), may hold values from -0.078125 to 0.078125
- up_weight: bfloat16 [4, 6144, 8192], P('sub', None, 'tp'), may hold values from -0.078125 to 0.078125
- down_weight: bfloat16 [4, 8192, 6144], P('sub', 'tp'), may hold values from -0.125 to 0.125
Outputs:
- layer_out: bfloat16 [128, 6144], P(('rep', 'sub'), 'tp'), parts along dimension 0
The draws below stay inside these ranges and needn't reach their ends.
There are 2 independent parts, one for each index of `rep`. The reference program is written for one: setup_inputs(seed, part) draws one part's arguments, and reference() takes and returns one part's arrays. A program takes and returns all parts, laid end to end along the dimension named above; an argument that names none is the same for every part. Nothing has to cross between parts.
Inputs may be any that keep to these rules, and one draw needn't show every extreme that they name: `routes`: the two experts of a row differ; within the 16 rows of one index of sub, no expert is named by more than 12 rows, a bound that some such block reaches.
All inputs are finite; a program needn't handle non-finite values.
Results may differ from the reference program's by a relative error of at most 0.0075.
Values may be sent and summed in bfloat16 or wider, within the bound.
A program may use at most 128 MiB of HBM per device.

```python
import math
import jax
import jax.numpy as jnp
import numpy as np
from jax import lax

D = 6144
H = 48
KVH = 8
HD = 128
FF = 8192
E = 4
SEQ_SUB = 16
B = 64
CACHE = 1024
MOST = 12


def draw_query(key, part):
    noise = jnp.clip(jax.random.normal(jax.random.fold_in(key, 1), (B, H * HD), jnp.float32), -6.0, 6.0)
    return noise.astype(jnp.bfloat16)


def draw_key_cache(key, part):
    noise = jnp.clip(jax.random.normal(jax.random.fold_in(key, 2), (B, CACHE, KVH * HD), jnp.float32), -6.0, 6.0)
    return noise.astype(jnp.bfloat16)


def draw_key_new(key, part):
    noise = jnp.clip(jax.random.normal(jax.random.fold_in(key, 3), (B, KVH * HD), jnp.float32), -6.0, 6.0)
    return noise.astype(jnp.bfloat16)


def draw_hidden_in(key, part):
    noise = jnp.clip(jax.random.normal(jax.random.fold_in(key, 4), (B, D), jnp.float32), -6.0, 6.0)
    column = jnp.arange(D).astype(jnp.float32)
    noise = noise * jnp.sqrt(1.0 + 2.0 * column / D)[None, :]
    return noise.astype(jnp.bfloat16)


def plant(values, rng, least, largest):
    longest = values.shape.index(max(values.shape))
    spots = []
    for shift in (0, 1):
        where = [jax.random.randint(jax.random.fold_in(rng, axis), (), 0, length) for axis, length in enumerate(values.shape)]
        where[longest] = (where[longest] + shift) % values.shape[longest]
        spots.append(tuple(where))
    return values.at[spots[0]].set(least).at[spots[1]].set(largest)


def strengthened(entries, own_key, source, target, parts, factor):
    owner, partner = [(jnp.arange(entries.shape[axis_at]) // (entries.shape[axis_at] // parts)).reshape([-1 if axis == axis_at else 1 for axis in range(entries.ndim)]) for axis_at in (source, target)]
    chosen = jax.random.permutation(own_key, parts)[partner]
    strong = (owner == chosen) | (owner == (partner + parts // 2) % parts)
    return jnp.where(strong, factor * entries, entries)


def level_of(key, dims, cuts, low, top_value):
    factor_of, own = 1.0, jax.random.fold_in(key, 6)
    for position, shards_of in cuts:
        draws = jnp.exp(jax.random.uniform(jax.random.fold_in(own, position), (shards_of,), jnp.float32, low / len(cuts), top_value / len(cuts)))
        factor_of = factor_of * jnp.repeat(draws, dims[position] // shards_of).reshape([-1 if axis == position else 1 for axis in range(len(dims))])
    return factor_of


def deal_out(key, own, number, rows, amount, top, most, slope):
    order = jax.random.permutation(key, amount)
    heavy_load, usual = shares(amount, rows * top, most, slope, True), shares(amount, rows * top, most, slope, False)
    places = jnp.arange(amount)

    def named(sizes, rotation):
        used = int((sizes > 0).sum())
        fixed = max(1, used // 4)
        passed = fixed + (places - fixed + rotation * (used - fixed)) % max(1, amount - fixed)
        return jnp.zeros((amount,), jnp.int32).at[order[jnp.where(places < fixed, places, passed)]].set(jnp.asarray(sizes, jnp.int32))

    sizes = jnp.where(number % 4 == 0, named(heavy_load, number // 4), named(usual, number - number // 4 - 1))
    mixed = jax.random.permutation(jax.random.fold_in(own, 3), amount)
    source_of, receiver = mixed[0:amount // 2 * 2:2], mixed[1:amount // 2 * 2:2]
    margin = jnp.minimum(sizes[source_of] - 1, most - sizes[receiver]) // 2
    margin = jnp.where((source_of == order[0]) | (receiver == order[0]) | (sizes[receiver] == 0), 0, jnp.maximum(margin, 0))
    passed = jax.random.randint(jax.random.fold_in(own, 4), (amount // 2,), 0, 1 << 20) % (margin + 1)
    sizes = sizes.at[source_of].add(-passed).at[receiver].add(passed)
    labels = jnp.searchsorted(jnp.cumsum(sizes), jnp.arange(rows * top), side="right").astype(jnp.int32)
    grid = labels.reshape(top, rows).T
    grid = grid[jax.random.permutation(jax.random.fold_in(own, 1), rows)]
    rotation = jax.random.randint(jax.random.fold_in(own, 2), (rows, 1), 0, top)
    return jnp.take_along_axis(grid, (jnp.arange(top)[None, :] + rotation) % top, axis=1)


def shares(number_of, total, bound, slope, full):
    loads = [(1 << 20) // math.isqrt(standing ** slope) + 1 for standing in range(1, number_of + 1)]
    largest = bound if full else min(bound, max(-(-total // number_of), total * loads[0] // sum(loads)))
    least = 1 if total - largest >= number_of - 1 else 0
    given, rest = [largest] + [least] * (number_of - 1), total - largest - least * (number_of - 1)
    while rest > 0:
        candidates = [i for i in range(1, number_of) if given[i] < largest] or [i for i in range(1, number_of) if given[i] < bound]
        mass, remaining = sum([loads[i] for i in candidates]), rest
        for i in candidates:
            addition = min(bound - given[i], max(1, remaining * loads[i] // mass), rest)
            given[i] = given[i] + addition
            rest = rest - addition
    return np.array(given)


def gaussian(own_key, dims, spread, bound, shards=(), held_as=jnp.bfloat16):
    array = spread * jax.random.normal(own_key, dims, jnp.float32)
    if shards:
        array = array * level_of(own_key, dims, shards, -0.22, 0.18)
    return jnp.clip(array, -bound, bound).astype(held_as)


def noise_with(own_key, dims, spread, reach, shards, heavy, kind=jnp.bfloat16):
    entries = spread * jax.random.normal(own_key, dims, jnp.float32)
    if shards:
        entries = entries * level_of(own_key, dims, shards, -0.22, 0.18)
    return jnp.clip(strengthened(entries, jax.random.fold_in(own_key, 3), *heavy), -reach, reach).astype(kind)


def setup_inputs(seed: int = 0, part: int = 0) -> dict:
    seeds = jax.random.split(jax.random.key(seed), 15)
    part_splits = jax.random.split(jax.random.fold_in(seeds[14], part), 15)
    hidden_in = draw_hidden_in(jax.random.fold_in(jax.random.fold_in(seeds[14], part), 71), part)
    query = draw_query(jax.random.fold_in(jax.random.fold_in(seeds[14], part), 71), part)
    key_new = draw_key_new(jax.random.fold_in(jax.random.fold_in(seeds[14], part), 71), part)
    value_new = gaussian(part_splits[3], (B, KVH * HD), 1.0, 6.0, ((0, 4), (1, 32)))
    key_cache = draw_key_cache(jax.random.fold_in(jax.random.fold_in(seeds[14], part), 71), part)
    value_cache = gaussian(part_splits[5], (B, CACHE, KVH * HD), 1.0, 6.0, ((0, 4), (1, 32)))
    lengths = plant(jax.random.randint(part_splits[6], (B,), 2, CACHE + 1), jax.random.fold_in(part_splits[6], 1), 2, CACHE).astype(jnp.int32)
    out_weight = gaussian(seeds[7], (H * HD, D), (H * HD) ** -0.5, 0.078125, ((0, 4), (1, 32)))
    norm_gain = jnp.clip(1.0 + 0.18 * jax.random.normal(seeds[8], (D,), jnp.float32), 0.099609375, 1.8984375).astype(jnp.bfloat16)
    router_weight = gaussian(seeds[9], (D, E), D ** -0.5, 0.078125, ((0, 32),))
    routes_keys = jax.random.split(jax.random.fold_in(part_splits[10], 1), B // SEQ_SUB)
    routes_turns = jax.random.permutation(jax.random.fold_in(part_splits[10], 3), B // SEQ_SUB)
    routes = jax.vmap(lambda own, number: deal_out(jax.random.fold_in(part_splits[10], 2), own, number, SEQ_SUB, E, 2, MOST, 2))(routes_keys, routes_turns).reshape((B, 2))
    gate_weight = gaussian(seeds[11], (E, D, FF), D ** -0.5, 0.078125, ((0, 4), (2, 32)))
    up_weight = gaussian(seeds[12], (E, D, FF), D ** -0.5, 0.078125, ((0, 4), (2, 32)))
    down_weight = noise_with(seeds[13], (E, FF, D), FF ** -0.5, 0.125, ((0, 4), (1, 32)), (1, 2, 32, 2.75))
    return dict(hidden_in=hidden_in, query=query, key_new=key_new, value_new=value_new, key_cache=key_cache, value_cache=value_cache, lengths=lengths, out_weight=out_weight, norm_gain=norm_gain, router_weight=router_weight, routes=routes, gate_weight=gate_weight, up_weight=up_weight, down_weight=down_weight)


def reference(hidden_in, query, key_new, value_new, key_cache, value_cache, lengths, out_weight, norm_gain, router_weight, routes, gate_weight, up_weight, down_weight):
    group_size = H // KVH
    scale_factor = 1.0 / HD ** 0.5
    query_rows = query.astype(jnp.float32).reshape(B, KVH, group_size, HD)
    cached_keys = key_cache.astype(jnp.float32).reshape(B, CACHE, KVH, HD)
    cached_values = value_cache.astype(jnp.float32).reshape(B, CACHE, KVH, HD)
    scores = jnp.einsum('bkgd,bpkd->bkgp', query_rows, cached_keys) * scale_factor
    valid = jnp.arange(CACHE, dtype=jnp.int32)[None, :] < lengths[:, None]
    scores = jnp.where(valid[:, None, None, :], scores, -jnp.inf)
    fresh_keys = key_new.astype(jnp.float32).reshape(B, KVH, HD)
    new_values = value_new.astype(jnp.float32).reshape(B, KVH, HD)
    owned_part = jnp.einsum('zyqn,zyn->zyq', query_rows, fresh_keys) * scale_factor
    run_max = jnp.maximum(lax.optimization_barrier(jnp.max(scores, axis=-1)), owned_part)
    weights = jnp.exp(scores - run_max[..., None])
    own_weight = jnp.exp(owned_part - run_max)
    total = lax.optimization_barrier(jnp.sum(weights, axis=-1)) + own_weight
    summed = jnp.einsum('bkgp,bpkd->bkgd', weights, cached_values) + own_weight[..., None] * new_values[:, :, None, :]
    attn = (summed / total[..., None]).reshape(B, H * HD).astype(jnp.bfloat16)
    resid = hidden_in.astype(jnp.float32) + jnp.dot(attn, out_weight, preferred_element_type=jnp.float32)
    root = jnp.sqrt(lax.optimization_barrier(jnp.mean(resid * resid, axis=-1, keepdims=True)) + 1e-05)
    normed = resid / root * norm_gain.astype(jnp.float32)
    normed_low = normed.astype(jnp.bfloat16)
    logits = jnp.dot(normed, router_weight.astype(jnp.float32), precision=lax.Precision.HIGHEST)
    expert_ids = jnp.arange(E, dtype=jnp.int32)[None, :]
    first_hot = (routes[:, 0:1] == expert_ids).astype(jnp.float32)
    second_hot = (routes[:, 1:2] == expert_ids).astype(jnp.float32)
    first_logit = lax.optimization_barrier(jnp.sum(logits * first_hot, axis=-1))
    second_logit = lax.optimization_barrier(jnp.sum(logits * second_hot, axis=-1))
    first_weight = 1.0 / (1.0 + jnp.exp(second_logit - first_logit))
    second_weight = 1.0 / (1.0 + jnp.exp(first_logit - second_logit))
    dense = first_weight[:, None] * first_hot + second_weight[:, None] * second_hot
    mixed = jnp.zeros((B, D), jnp.float32)
    for expert in range(E):
        gate_out = jnp.dot(normed_low, gate_weight[expert], preferred_element_type=jnp.float32)
        up_out = jnp.dot(normed_low, up_weight[expert], preferred_element_type=jnp.float32)
        inner = (jax.nn.silu(gate_out) * up_out).astype(jnp.bfloat16)
        result = jnp.dot(inner, down_weight[expert], preferred_element_type=jnp.float32)
        mixed = mixed + dense[:, expert:expert + 1] * result
    return (resid + mixed).astype(jnp.bfloat16)
```

```python
import functools

import jax
import jax.numpy as jnp
from jax import lax
from jax.experimental import pallas as pl
from jax.experimental.pallas import tpu as pltpu
from jax.sharding import PartitionSpec as P

HD = 128
F32 = jnp.float32
BF16 = jnp.bfloat16
MESH = pl.DeviceIdType.MESH
FLOOR = -1e30


def lanes(shape):
    return lax.broadcasted_iota(jnp.int32, shape, len(shape) - 1)


def pick(flag, first, second):
    return jnp.where(jnp.full(first.shape, flag, jnp.int32) == 0, first, second)


def joined(a0, a1, b0, b1):
    lane = lanes(a0.shape)
    r0, r1 = pltpu.roll(b0, 64, 1), pltpu.roll(b1, 64, 1)
    return a0, jnp.where(lane < 64, a1, r0), jnp.where(lane < 64, r0, r1)


def layer(
    Z, X, D, P_LOC,
    pk, gr, lens, routes, kc, vc, wo, gw, uw, dw,
    out,
    ppk, pgr, kbuf, vbuf, wbuf, gbuf, ubuf, dbuf,
    kvt, kvo, qbuf, obuf, rbuf, abuf, axb, pbuf, prs, prb,
    hbuf, tbuf, irb, inner, ysend, yrecv, ymine, xsend, xrecv, acc, zsend, zrecv, fsend, frecv,
    lsem, dss, dsr, qs, qr, kvs, kvr, os_, or_, as_, ar, axs, axr, prss, prsr,
    hs, hr, ts, tr, hxs, hxr, hds, hdr, ixs, ixr, ids, idr, ys, yr, xs, xr, zs, zr, fs, fr,
):
    t = lax.axis_index("tp")
    s = lax.axis_index("sub")
    c = t % 2
    z = t // 2
    o = 1 - c
    partner = t + 1 - 2 * c
    CW = 3 * HD
    KVH = Z // 2
    DX = D // X
    scale = 1.0 / HD**0.5

    def remote(src, dst, ssem, rsem, **where):
        return pltpu.make_async_remote_copy(
            src_ref=src, dst_ref=dst, send_sem=ssem, recv_sem=rsem,
            device_id=where, device_id_type=MESH,
        )

    def over_z(fn):
        def step(k, carry):
            d = Z // 2 + jnp.where(k % 2 == 0, k // 2, -((k + 1) // 2))
            fn(d)
            return carry

        lax.fori_loop(0, Z - 1, step, 0)

    def chip(i, width):
        return pl.ds(pl.multiple_of(i * width, 128), width)

    half = pl.ds(pl.multiple_of(8 * c, 8), 8)
    other = pl.ds(pl.multiple_of(8 * o, 8), 8)
    local = [
        pltpu.make_async_copy(kc.at[half], kbuf.at[c], lsem.at[0]),
        pltpu.make_async_copy(vc.at[half], vbuf.at[c], lsem.at[1]),
        pltpu.make_async_copy(wo, wbuf.at[c], lsem.at[2]),
        pltpu.make_async_copy(gw.at[0], gbuf, lsem.at[3]),
        pltpu.make_async_copy(uw.at[0], ubuf, lsem.at[4]),
        pltpu.make_async_copy(dw.at[0], dbuf, lsem.at[5]),
    ]
    for copy in local:
        copy.start()

    barrier = pltpu.get_barrier_semaphore()

    def greet(d):
        pl.semaphore_signal(
            barrier, inc=1, device_id={"tp": 2 * ((z + d) % Z) + c}, device_id_type=MESH
        )

    over_z(greet)
    for d in range(1, X):
        pl.semaphore_signal(barrier, inc=1, device_id={"sub": (s + d) % X}, device_id_type=MESH)
    pl.semaphore_signal(barrier, inc=1, device_id={"tp": partner}, device_id_type=MESH)
    pl.semaphore_wait(barrier, Z - 1 + X - 1 + 1)

    swaps = [
        remote(pk.at[o], ppk, dss.at[0], dsr.at[0], tp=partner),
        remote(gr, pgr, dss.at[1], dsr.at[1], tp=partner),
        remote(kc.at[other], kbuf.at[c], dss.at[2], dsr.at[2], tp=partner),
        remote(vc.at[other], vbuf.at[c], dss.at[3], dsr.at[3], tp=partner),
        remote(wo, wbuf.at[c], dss.at[4], dsr.at[4], tp=partner),
    ]
    for copy in swaps:
        copy.start()
    swaps[0].wait_recv()

    mine = pk[c].astype(F32)
    theirs = ppk[...].astype(F32)
    first, second = pick(c, mine, theirs), pick(c, theirs, mine)
    lane = lanes((8, HD))

    def tile(value, k):
        return value[:, HD * k : HD * (k + 1)]

    q_own = joined(tile(first, 0), tile(first, 1), tile(second, 0), tile(second, 1))
    hid = joined(tile(first, 2), tile(first, 3), tile(second, 2), tile(second, 3))
    qbuf[:, chip(z, CW)] = jnp.concatenate(q_own, axis=1).astype(BF16)

    def send_q(d):
        to = (z + d) % Z
        remote(
            qbuf.at[:, chip(z, CW)], qbuf.at[:, chip(z, CW)], qs.at[to], qr.at[z], tp=2 * to + c
        ).start()

    over_z(send_q)
    kvt[...] = jnp.where(lane < 64, pltpu.roll(tile(first, 1), 64, 1), tile(second, 1)).astype(BF16)
    z_pair = z + 1 - 2 * (z % 2)
    kv_copy = remote(kvt, kvo, kvs.at[0], kvr.at[0], tp=2 * z_pair + c)
    kv_copy.start()

    local[0].wait()
    local[1].wait()
    swaps[2].wait_recv()
    swaps[3].wait_recv()

    def wait_q(d):
        at = (z + d) % Z
        remote(
            qbuf.at[:, chip(at, CW)], qbuf.at[:, chip(at, CW)], qs.at[at], qr.at[at], tp=2 * at + c
        ).wait_recv()

    over_z(wait_q)

    cols = 2 * 8 * P_LOC
    group = 6
    rows = group * 8
    col = lax.broadcasted_iota(jnp.int32, (rows, cols), 1)
    row = lax.broadcasted_iota(jnp.int32, (rows, cols), 0)
    position = (2 * z + col // (8 * P_LOC)) * P_LOC + col % P_LOC
    length = jnp.concatenate([jnp.broadcast_to(lens[half, :], (8, cols))] * group, axis=0)
    valid = (row % 8 == (col % (8 * P_LOC)) // P_LOC) & (position < length)
    for g in range(KVH):
        at = slice(HD * g, HD * (g + 1))
        q_g = qbuf[:, group * HD * g : group * HD * (g + 1)].astype(F32)
        q_g = jnp.concatenate([tile(q_g, i) for i in range(group)], axis=0).astype(BF16)
        keys = kbuf[:, :, :, at].reshape(cols, HD)
        values = vbuf[:, :, :, at].reshape(cols, HD)
        scores = (
            lax.dot_general(q_g, keys, (((1,), (1,)), ((), ())), preferred_element_type=F32) * scale
        )
        scores = jnp.where(valid, scores, FLOOR)
        top = jnp.max(scores, axis=1, keepdims=True).astype(BF16).astype(F32)
        weights = jnp.where(valid, jnp.exp(scores - top), 0.0)
        total = jnp.sum(weights, axis=1, keepdims=True)
        summed = jnp.dot(weights.astype(BF16), values, preferred_element_type=F32)
        high = total.astype(BF16).astype(F32)
        low = total - high
        for k in range(2):
            stats = jnp.zeros((8, HD), F32)
            parts = []
            for j in range(3):
                at_row = slice(8 * (3 * k + j), 8 * (3 * k + j + 1))
                parts.append(summed[at_row])
                stats = jnp.where(lane == j, top[at_row], stats)
                stats = jnp.where(lane == 32 + j, high[at_row], stats)
                stats = jnp.where(lane == 64 + j, low[at_row], stats)
            block = jnp.concatenate(parts + [stats], axis=1).astype(BF16)
            obuf[:, 4 * HD * (2 * g + k) : 4 * HD * (2 * g + k + 1)] = block

    def send_o(d):
        to = (z + d) % Z
        remote(
            obuf.at[:, chip(to, 4 * HD)], rbuf.at[z], os_.at[to], or_.at[z], tp=2 * to + c
        ).start()

    over_z(send_o)
    rbuf[z] = obuf[:, chip(z, 4 * HD)]
    kv_copy.wait_recv()
    t_mine, t_pair = kvt[...].astype(F32), kvo[...].astype(F32)
    even, odd = pick(z % 2, t_mine, t_pair), pick(z % 2, t_pair, t_mine)

    def quarters(shifts):
        w = [pltpu.roll(v, k, 1) if k else v for v, k in zip((even, even, odd, odd), shifts)]
        low_half = jnp.where(lane < 32, w[0], w[1])
        high_half = jnp.where(lane < 96, w[2], w[3])
        return jnp.where(lane < 64, low_half, high_half)

    key_own = quarters((0, 96, 64, 32))
    value_own = quarters((96, 64, 32, 0))
    own = jnp.zeros((8, HD), F32)
    for j in range(3):
        dot = jnp.sum(q_own[j] * key_own, axis=1, keepdims=True) * scale
        own = jnp.where(lane == j, dot, own)

    def wait_o(d):
        at = (z + d) % Z
        remote(
            obuf.at[:, chip(at, 4 * HD)], rbuf.at[at], os_.at[at], or_.at[at], tp=2 * at + c
        ).wait_recv()

    over_z(wait_o)
    tops = [rbuf[k, :, 3 * HD :].astype(F32) for k in range(Z)]
    top = own
    for part in tops:
        top = jnp.maximum(top, part)
    own_weight = jnp.where(lane < 3, jnp.exp(own - top), 0.0)
    total = own_weight
    factors = []
    for part in tops:
        factor = jnp.where(lane < 3, jnp.exp(part - top), 0.0)
        factors.append(factor)
        total = total + factor * (pltpu.roll(part, 96, 1) + pltpu.roll(part, 64, 1))
    inverse = jnp.where(lane < 3, 1.0 / jnp.where(lane < 3, total, 1.0), 0.0)
    own_weight = own_weight * inverse
    parts = []
    for j in range(3):
        value = own_weight[:, j : j + 1] * value_own
        for k in range(Z):
            factor = factors[k] * inverse
            value = value + factor[:, j : j + 1] * rbuf[k, :, HD * j : HD * (j + 1)].astype(F32)
        parts.append(value)
    abuf[:, chip(z, CW)] = jnp.concatenate(parts, axis=1).astype(BF16)

    def send_a(d):
        to = (z + d) % Z
        remote(
            abuf.at[:, chip(z, CW)], abuf.at[:, chip(z, CW)], as_.at[to], ar.at[z], tp=2 * to + c
        ).start()

    over_z(send_a)
    local[2].wait()
    swaps[1].wait_recv()
    swaps[4].wait_recv()

    def wait_a(d):
        at = (z + d) % Z
        remote(
            abuf.at[:, chip(at, CW)], abuf.at[:, chip(at, CW)], as_.at[at], ar.at[at], tp=2 * at + c
        ).wait_recv()

    over_z(wait_a)

    def x_copy(d, src, dst, ssem, rsem, frm=False):
        to = (s + d) % X
        return remote(src(to), dst(to if frm else s), ssem.at[to], rsem.at[to if frm else s], sub=to)

    def attn_copy(d, frm=False):
        return x_copy(
            d, lambda to: abuf.at[:, chip(to, DX)], lambda at: axb.at[at], axs, axr, frm
        )

    for d in range(1, X):
        attn_copy(d).start()
    axb[s] = abuf[:, chip(s, DX)]
    for d in range(1, X):
        attn_copy(d, True).wait_recv()
    left = axb[...].astype(F32).reshape(8 * X, DX).astype(BF16)
    for k in range(2):
        pbuf[k, :, HD:] = jnp.zeros((8 * X, HD), F32)
        pbuf[k, :, : D // (2 * Z)] = jnp.dot(left, wbuf[k], preferred_element_type=F32)
    both = [pbuf[k] for k in range(2)]
    tiles = joined(tile(both[0], 0), tile(both[0], 1), tile(both[1], 0), tile(both[1], 1))
    prs[...] = jnp.concatenate(tiles, axis=1).reshape(X, 8, CW)

    def proj_copy(d, frm=False):
        return x_copy(d, lambda to: prs.at[to], lambda at: prb.at[at], prss, prsr, frm)

    for d in range(1, X):
        proj_copy(d).start()
    resid = jnp.concatenate(hid, axis=1) + prs[s]
    g_mine, g_theirs = gr[...], pgr[...]
    ga, gb = pick(c, g_mine, g_theirs), pick(c, g_theirs, g_mine)
    gains = jnp.concatenate(joined(tile(ga, 0), tile(ga, 1), tile(gb, 0), tile(gb, 1)), axis=1)
    for d in range(1, X):
        proj_copy(d, True).wait_recv()
        resid = resid + prb[(s + d) % X]
    gained = resid * gains[0:1]
    hbuf[c, s, :, chip(z, CW)] = gained.astype(BF16)
    stats = jnp.where(lane == 0, jnp.sum(resid * resid, axis=1, keepdims=True), 0.0)
    for e in range(X):
        logit = jnp.sum(gained * gains[e + 1 : e + 2], axis=1, keepdims=True)
        stats = jnp.where(lane == e + 1, logit, stats)
    tbuf[z] = stats

    def h_copy(d):
        to = (z + d) % Z
        return remote(
            hbuf.at[c, s, :, chip(z, CW)], hbuf.at[c, s, :, chip(z, CW)],
            hs.at[to], hr.at[z], tp=2 * to + c,
        )

    def t_copy(d):
        to = (z + d) % Z
        return remote(tbuf.at[z], tbuf.at[z], ts.at[to], tr.at[z], tp=2 * to + c)

    over_z(lambda d: t_copy(d).start())
    over_z(lambda d: h_copy(d).start())

    def wait_t(d):
        at = (z + d) % Z
        remote(tbuf.at[at], tbuf.at[at], ts.at[at], tr.at[at], tp=2 * at + c).wait_recv()

    over_z(wait_t)
    sums = tbuf[0]
    for k in range(1, Z):
        sums = sums + tbuf[k]
    inv_root = 1.0 / jnp.sqrt(sums[:, 0:1] / D + 1e-05)
    irb[c, s] = jnp.broadcast_to(inv_root, (8, HD))

    def h_x(d, frm=False):
        at = (s + d) % X
        src = at if frm else s
        return (
            remote(hbuf.at[c, src], hbuf.at[c, src], hxs.at[at], hxr.at[src], sub=at),
            remote(irb.at[c, src], irb.at[c, src], ixs.at[at], ixr.at[src], sub=at),
        )

    def h_d(src, core):
        return (
            remote(hbuf.at[core, src], hbuf.at[core, src], hds.at[src], hdr.at[src], tp=partner),
            remote(irb.at[core, src], irb.at[core, src], ids.at[src], idr.at[src], tp=partner),
        )

    for d in range(1, X):
        h_x(d)[1].start()
    h_d(s, c)[1].start()
    logits = sums * inv_root
    picked = routes[half, :]
    hot_first, hot_second = lane == picked[:, 0:1] + 1, lane == picked[:, 1:2] + 1
    l_first = jnp.sum(jnp.where(hot_first, logits, 0.0), axis=1, keepdims=True)
    l_second = jnp.sum(jnp.where(hot_second, logits, 0.0), axis=1, keepdims=True)
    w_first = 1.0 / (1.0 + jnp.exp(l_second - l_first))
    w_second = 1.0 / (1.0 + jnp.exp(l_first - l_second))
    dense = jnp.where(hot_first, w_first, 0.0) + jnp.where(hot_second, w_second, 0.0)

    def share(e):
        return jnp.sum(jnp.where(lane == e + 1, dense, 0.0), axis=1, keepdims=True)

    def wait_h(d):
        at = (z + d) % Z
        remote(
            hbuf.at[c, s, :, chip(at, CW)], hbuf.at[c, s, :, chip(at, CW)],
            hs.at[at], hr.at[at], tp=2 * at + c,
        ).wait_recv()

    over_z(wait_h)
    for d in range(1, X):
        h_x(d)[0].start()
    h_d(s, c)[0].start()
    for d in range(1, X):
        for k in (1, 0):
            h_x(d, True)[k].wait_recv()
            h_d((s + d) % X, c)[k].start()
    for d in range(X):
        for k in (1, 0):
            h_d((s + d) % X, o)[k].wait_recv()
    for copy in local[3:]:
        copy.wait()

    N = 16 * X
    F = gbuf.shape[1]
    step = 6 * HD
    gate = jnp.zeros((N, F), F32)
    up = jnp.zeros((N, F), F32)
    for k in range(0, D, step):
        left = hbuf[:, :, :, k : k + step].astype(F32).reshape(N, step).astype(BF16)
        gate = gate + jnp.dot(left, gbuf[k : k + step], preferred_element_type=F32)
        up = up + jnp.dot(left, ubuf[k : k + step], preferred_element_type=F32)
    inv = irb[...].reshape(N, HD)
    inv = jnp.concatenate([inv] * (F // HD), axis=1)
    gate, up = gate * inv, up * inv
    inner[...] = (gate / (1.0 + jnp.exp(-gate)) * up).reshape(2, N // 2, F).astype(BF16)
    left = inner[o]
    for k in range(0, D, step):
        part = jnp.dot(left, dbuf[:, k : k + step], preferred_element_type=F32)
        ysend[:, :, k : k + step] = part.reshape(X, 8, step).astype(BF16)
    y_copy = remote(ysend, yrecv, ys.at[0], yr.at[0], tp=partner)
    y_copy.start()
    left = inner[c]
    for k in range(0, D, step):
        part = jnp.dot(left, dbuf[:, k : k + step], preferred_element_type=F32)
        ymine[:, :, k : k + step] = part.reshape(X, 8, step)
    y_copy.wait_recv()

    def y_x(d, frm=False):
        return x_copy(d, lambda to: xsend.at[to], lambda at: xrecv.at[at], xs, xr, frm)

    for d in range(1, X):
        to = (s + d) % X
        xsend[to] = (ymine[to] + yrecv[to].astype(F32)).astype(BF16)
        y_x(d).start()
    acc[...] = share(s) * (ymine[s] + yrecv[s].astype(F32))
    for d in range(1, X):
        y_x(d, True).wait_recv()
        at = (s + d) % X
        acc[...] += share(at) * xrecv[at].astype(F32)
    zsend[...] = acc[...].astype(BF16)

    def send_z(d):
        to = (z + d) % Z
        remote(
            zsend.at[:, chip(to, CW)], zrecv.at[z], zs.at[to], zr.at[z], tp=2 * to + c
        ).start()

    over_z(send_z)
    zrecv[z] = jnp.zeros((8, CW), BF16)
    result = resid + acc[:, chip(z, CW)]

    def wait_z(d):
        at = (z + d) % Z
        remote(
            zsend.at[:, chip(at, CW)], zrecv.at[at], zs.at[at], zr.at[at], tp=2 * at + c
        ).wait_recv()

    over_z(wait_z)
    for k in range(Z):
        result = result + zrecv[k].astype(F32)

    r1, r2 = pltpu.roll(tile(result, 1), 64, 1), pltpu.roll(tile(result, 2), 64, 1)
    v_first = result[:, : 2 * HD]
    v_second = jnp.concatenate([jnp.where(lane < 64, r1, r2), r2], axis=1)
    fsend[...] = pick(c, v_second, v_first).astype(BF16)
    f_copy = remote(fsend, frecv, fs.at[0], fr.at[0], tp=partner)
    f_copy.start()
    kept = pick(c, v_first, v_second)

    def sent(d):
        to = (z + d) % Z
        for src, ssem in (
            (qbuf.at[:, chip(z, CW)], qs), (obuf.at[:, chip(to, 4 * HD)], os_),
            (abuf.at[:, chip(z, CW)], as_), (hbuf.at[c, s, :, chip(z, CW)], hs),
            (tbuf.at[z], ts), (zsend.at[:, chip(to, CW)], zs),
        ):
            remote(src, src, ssem.at[to], qr.at[z], tp=2 * to + c).wait_send()

    over_z(sent)
    for copy in swaps:
        copy.wait_send()
    kv_copy.wait_send()
    y_copy.wait_send()
    for d in range(1, X):
        attn_copy(d).wait_send()
        proj_copy(d).wait_send()
        y_x(d).wait_send()
        for copy in h_x(d):
            copy.wait_send()
    for d in range(X):
        for copy in h_d((s + d) % X, c):
            copy.wait_send()
    f_copy.wait()
    came = frecv[...].astype(F32)
    whole = jnp.concatenate([pick(c, kept, came), pick(c, came, kept)], axis=0)
    out[...] = whole[:, : D // (2 * Z)].astype(BF16)


def on_device(
    Z, X,
    hidden_in, query, key_new, value_new, key_cache, value_cache, lengths,
    out_weight, norm_gain, router_weight, routes, gate_weight, up_weight, down_weight,
):
    width = hidden_in.shape[1]
    D = width * 2 * Z
    P_LOC = key_cache.shape[1]
    F = gate_weight.shape[2]
    CW = 3 * HD
    pk = jnp.concatenate([query, key_new, value_new, hidden_in], axis=1)
    pk = jnp.pad(pk, ((0, 0), (0, 4 * HD - pk.shape[1]))).reshape(2, 8, 4 * HD)
    gr = jnp.concatenate([norm_gain[None].astype(F32), router_weight.astype(F32).T], axis=0)
    gr = jnp.pad(gr, ((0, 8 - gr.shape[0]), (0, 2 * HD - width)))
    vm = pl.BlockSpec(memory_space=pltpu.VMEM)
    anywhere = pl.BlockSpec(memory_space=pl.ANY)
    dma = pltpu.SemaphoreType.DMA
    V = pltpu.VMEM
    scratch = [
        V((8, 4 * HD), BF16), V((8, 2 * HD), F32),
        V((2, 8, P_LOC, key_cache.shape[2]), BF16), V((2, 8, P_LOC, key_cache.shape[2]), BF16),
        V((2, *out_weight.shape), BF16),
        V((D, F), BF16), V((D, F), BF16), V((F, D), BF16),
        V((8, HD), BF16), V((8, HD), BF16),
        V((8, D), BF16),
        V((8, Z * 4 * HD), BF16), V((Z, 8, 4 * HD), BF16),
        V((8, D), BF16), V((X, 8, D // X), BF16),
        V((2, 8 * X, 2 * HD), F32), V((X, 8, CW), F32), V((X, 8, CW), F32),
        V((2, X, 8, D), BF16), V((Z, 8, HD), F32), V((2, X, 8, HD), F32),
        V((2, 8 * X, F), BF16),
        V((X, 8, D), BF16), V((X, 8, D), BF16), V((X, 8, D), F32),
        V((X, 8, D), BF16), V((X, 8, D), BF16),
        V((8, D), F32), V((8, D), BF16), V((Z, 8, CW), BF16),
        V((8, 2 * HD), BF16), V((8, 2 * HD), BF16),
        dma((6,)), dma((5,)), dma((5,)),
        dma((Z,)), dma((Z,)), dma((1,)), dma((1,)),
        dma((Z,)), dma((Z,)), dma((Z,)), dma((Z,)),
        dma((X,)), dma((X,)), dma((X,)), dma((X,)),
        dma((Z,)), dma((Z,)), dma((Z,)), dma((Z,)),
        dma((X,)), dma((X,)), dma((X,)), dma((X,)), dma((X,)), dma((X,)), dma((X,)), dma((X,)),
        dma((1,)), dma((1,)), dma((X,)), dma((X,)), dma((Z,)), dma((Z,)), dma((1,)), dma((1,)),
    ]
    return pl.pallas_call(
        functools.partial(layer, Z, X, D, P_LOC),
        out_shape=jax.ShapeDtypeStruct(hidden_in.shape, BF16),
        in_specs=[vm] * 4 + [anywhere] * 6,
        out_specs=vm,
        scratch_shapes=scratch,
        compiler_params=pltpu.CompilerParams(
            collective_id=0, has_side_effects=True, vmem_limit_bytes=56 * 1024 * 1024
        ),
        name="decode_layer",
    )(
        pk, gr, lengths[:, None], routes, key_cache, value_cache, out_weight,
        gate_weight, up_weight, down_weight,
    )


def solution(mesh):
    Z, X = mesh.shape["tp"] // 2, mesh.shape["sub"]
    rows = P(("rep", "sub"), "tp")
    return jax.shard_map(
        functools.partial(on_device, Z, X),
        mesh=mesh,
        in_specs=(
            rows, rows, rows, rows,
            P(("rep", "sub"), "tp", None), P(("rep", "sub"), "tp", None), P(("rep", "sub")),
            P("sub", "tp"), P("tp"), P("tp", None), P(("rep", "sub"), None),
            P("sub", None, "tp"), P("sub", None, "tp"), P("sub", "tp", None),
        ),
        out_specs=rows,
        check_vma=False,
    )
```

```python
import functools

import jax
import jax.numpy as jnp
from jax import lax
from jax.experimental import pallas as pl
from jax.experimental.pallas import tpu as pltpu
from jax.sharding import PartitionSpec as P

HD = 128
F32 = jnp.float32
BF16 = jnp.bfloat16
MESH = pl.DeviceIdType.MESH
FLOOR = -1e30
CHUNKS = 4
SEMAPHORES = 96


def lanes(shape):
    return lax.broadcasted_iota(jnp.int32, shape, len(shape) - 1)


def pick(flag, first, second):
    return jnp.where(jnp.full(first.shape, flag, jnp.int32) == 0, first, second)


def joined(a0, a1, b0, b1):
    lane = lanes(a0.shape)
    r0, r1 = pltpu.roll(b0, 64, 1), pltpu.roll(b1, 64, 1)
    return a0, jnp.where(lane < 64, a1, r0), jnp.where(lane < 64, r0, r1)


def layer(
    Z, X, D, P_LOC,
    hidden, query, k_new, v_new, lens, routes, gain, router, kc, vc, wo, gw, uw, dw,
    out,
    phid, pq, pk, pv, pgain, prouter, small,
    kbuf, vbuf, wbuf, gbuf, ubuf, dbuf,
    kvt, kvo, qbuf, obuf, rbuf, abuf, pbuf,
    hbuf, tbuf, irb, inner, ysend, yrecv, ymine, xsend, xrecv, acc, zsend, zrecv, fsend, frecv,
    lsem, sems,
):
    t = lax.axis_index("tp")
    s = lax.axis_index("sub")
    c = t % 2
    z = t // 2
    o = 1 - c
    partner = t + 1 - 2 * c
    CW = 3 * HD
    KVH = Z // 2
    DX = D // X
    taken = iter(range(SEMAPHORES))
    scale = 1.0 / HD**0.5

    def sem():
        return sems.at[next(taken)]

    def remote(src, dst, ssem, rsem, **where):
        return pltpu.make_async_remote_copy(
            src_ref=src, dst_ref=dst, send_sem=ssem, recv_sem=rsem,
            device_id=where, device_id_type=MESH,
        )

    def over_z(fn):
        def step(k, carry):
            d = Z // 2 + jnp.where(k % 2 == 0, k // 2, -((k + 1) // 2))
            fn((z + d) % Z)
            return carry

        lax.fori_loop(0, Z - 1, step, 0)

    def z_phase(src, dst, width):
        ssem, rsem = sem(), sem()

        def send(to):
            remote(src(to), dst, ssem, rsem, tp=2 * to + c).start()

        over_z(send)
        return ssem, rsem

    def block_wait(ref, ssem, rsem):
        return remote(ref, ref, ssem, rsem, tp=partner)

    def chip(i, width):
        return pl.ds(pl.multiple_of(i * width, 128), width)

    half = pl.ds(pl.multiple_of(8 * c, 8), 8)
    other = pl.ds(pl.multiple_of(8 * o, 8), 8)
    local = [
        pltpu.make_async_copy(kc.at[half], kbuf.at[c], lsem.at[0]),
        pltpu.make_async_copy(vc.at[half], vbuf.at[c], lsem.at[1]),
        pltpu.make_async_copy(wo, wbuf.at[c, s], lsem.at[2]),
        pltpu.make_async_copy(gw.at[0], gbuf, lsem.at[3]),
        pltpu.make_async_copy(uw.at[0], ubuf, lsem.at[4]),
        pltpu.make_async_copy(dw.at[0], dbuf, lsem.at[5]),
    ]
    for copy in local:
        copy.start()

    barrier = pltpu.get_barrier_semaphore()

    def greet(to):
        pl.semaphore_signal(barrier, inc=1, device_id={"tp": 2 * to + c}, device_id_type=MESH)

    over_z(greet)
    for d in range(1, X):
        pl.semaphore_signal(barrier, inc=1, device_id={"sub": (s + d) % X}, device_id_type=MESH)
    pl.semaphore_signal(barrier, inc=1, device_id={"tp": partner}, device_id_type=MESH)
    pl.semaphore_wait(barrier, Z - 1 + X - 1 + 1)

    swaps = [
        remote(src, dst, sem(), sem(), tp=partner)
        for src, dst in (
            (query.at[other], pq), (k_new.at[other], pk), (v_new.at[other], pv),
            (hidden.at[other], phid), (gain, pgain), (router, prouter),
            (kc.at[other], kbuf.at[c]), (vc.at[other], vbuf.at[c]), (wo, wbuf.at[c, s]),
        )
    ]
    for copy in swaps:
        copy.start()
    w_x = [
        remote(wo, wbuf.at[c, s], sem(), sem(), sub=(s + d) % X) for d in range(1, X)
    ]
    for copy in w_x:
        copy.start()
    lane = lanes((8, HD))

    def tile(value, k):
        return value[:, HD * k : HD * (k + 1)]

    def widened(*parts):
        pairs = []
        for k, part in enumerate(parts):
            small[k, : part.shape[0], : part.shape[1]] = part.astype(F32)
            pairs.append((small[k, :, :HD], small[k, :, HD:]))
        return pairs

    def chip_tiles(own, came):
        (o0, o1), (c0, c1) = widened(own, came)
        return joined(pick(c, o0, c0), pick(c, o1, c1), pick(c, c0, o0), pick(c, c1, o1))

    small[...] = jnp.zeros(small.shape, F32)
    swaps[0].wait_recv()

    q_own = chip_tiles(query[half, :], pq[...])
    qbuf[:, chip(z, CW)] = jnp.concatenate(q_own, axis=1).astype(BF16)

    own_q = qbuf.at[:, chip(z, CW)]
    q_sems = z_phase(lambda to: own_q, own_q, CW)
    for copy in swaps[1:6]:
        copy.wait_recv()
    small[...] = jnp.zeros(small.shape, F32)
    kv = [v[0] for v in widened(k_new[half, :], v_new[half, :], pk[...], pv[...])]
    kv = [pick(c, kv[0], kv[2]), pick(c, kv[1], kv[3]), pick(c, kv[2], kv[0]), pick(c, kv[3], kv[1])]
    kv = [kv[0]] + [pltpu.roll(v, 32 * (k + 1), 1) for k, v in enumerate(kv[1:])]
    kvt[...] = (kv[0] + kv[1] + kv[2] + kv[3]).astype(BF16)
    z_pair = z + 1 - 2 * (z % 2)
    kv_copy = remote(kvt, kvo, sem(), sem(), tp=2 * z_pair + c)
    kv_copy.start()

    local[0].wait()
    local[1].wait()
    swaps[6].wait_recv()
    swaps[7].wait_recv()

    all_q = block_wait(qbuf.at[:, : (Z - 1) * CW], *q_sems)
    all_q.wait_recv()

    cols = 2 * 8 * P_LOC
    group = 6
    rows = group * 8
    col = lax.broadcasted_iota(jnp.int32, (rows, cols), 1)
    row = lax.broadcasted_iota(jnp.int32, (rows, cols), 0)
    position = (2 * z + col // (8 * P_LOC)) * P_LOC + col % P_LOC
    spread = lax.broadcasted_iota(jnp.int32, (8, 16), 1)
    chosen = spread == lax.broadcasted_iota(jnp.int32, (8, 16), 0) + 8 * c

    def column(line):
        picked = jnp.where(chosen, jnp.broadcast_to(line.astype(F32), (8, 16)), 0.0)
        return jnp.sum(picked, axis=1, keepdims=True).astype(jnp.int32)

    length = jnp.broadcast_to(column(lens[...]), (8, cols))
    length = jnp.concatenate([length] * group, axis=0)
    valid = (row % 8 == (col % (8 * P_LOC)) // P_LOC) & (position < length)
    for g in range(KVH):
        at = slice(HD * g, HD * (g + 1))
        q_g = qbuf[:, group * HD * g : group * HD * (g + 1)].astype(F32)
        q_g = jnp.concatenate([tile(q_g, i) for i in range(group)], axis=0).astype(BF16)
        keys = kbuf[:, :, :, at].reshape(cols, HD)
        values = vbuf[:, :, :, at].reshape(cols, HD)
        scores = (
            lax.dot_general(q_g, keys, (((1,), (1,)), ((), ())), preferred_element_type=F32) * scale
        )
        scores = jnp.where(valid, scores, FLOOR)
        top = jnp.max(scores, axis=1, keepdims=True).astype(BF16).astype(F32)
        weights = jnp.where(valid, jnp.exp(scores - top), 0.0)
        total = jnp.sum(weights, axis=1, keepdims=True)
        summed = jnp.dot(weights.astype(BF16), values, preferred_element_type=F32)
        high = total.astype(BF16).astype(F32)
        low = total - high
        for k in range(2):
            stats = jnp.zeros((8, HD), F32)
            parts = []
            for j in range(3):
                at_row = slice(8 * (3 * k + j), 8 * (3 * k + j + 1))
                parts.append(summed[at_row])
                stats = jnp.where(lane == j, top[at_row], stats)
                stats = jnp.where(lane == 32 + j, high[at_row], stats)
                stats = jnp.where(lane == 64 + j, low[at_row], stats)
            block = jnp.concatenate(parts + [stats], axis=1).astype(BF16)
            obuf[:, 4 * HD * (2 * g + k) : 4 * HD * (2 * g + k + 1)] = block

    o_sems = z_phase(lambda to: obuf.at[:, chip(to, 4 * HD)], rbuf.at[z], 4 * HD)
    rbuf[z] = obuf[:, chip(z, 4 * HD)]
    kv_copy.wait_recv()
    t_mine, t_pair = kvt[...].astype(F32), kvo[...].astype(F32)
    even, odd = pick(z % 2, t_mine, t_pair), pick(z % 2, t_pair, t_mine)

    def quarters(shifts):
        w = [pltpu.roll(v, k, 1) if k else v for v, k in zip((even, even, odd, odd), shifts)]
        low_half = jnp.where(lane < 32, w[0], w[1])
        high_half = jnp.where(lane < 96, w[2], w[3])
        return jnp.where(lane < 64, low_half, high_half)

    key_own = quarters((0, 96, 64, 32))
    value_own = quarters((96, 64, 32, 0))
    own = jnp.zeros((8, HD), F32)
    for j in range(3):
        dot = jnp.sum(q_own[j] * key_own, axis=1, keepdims=True) * scale
        own = jnp.where(lane == j, dot, own)

    all_o = block_wait(rbuf.at[: Z - 1], *o_sems)
    all_o.wait_recv()
    tops = [rbuf[k, :, 3 * HD :].astype(F32) for k in range(Z)]
    top = own
    for part in tops:
        top = jnp.maximum(top, part)
    own_weight = jnp.where(lane < 3, jnp.exp(own - top), 0.0)
    total = own_weight
    factors = []
    for part in tops:
        factor = jnp.where(lane < 3, jnp.exp(part - top), 0.0)
        factors.append(factor)
        total = total + factor * (pltpu.roll(part, 96, 1) + pltpu.roll(part, 64, 1))
    inverse = jnp.where(lane < 3, 1.0 / jnp.where(lane < 3, total, 1.0), 0.0)
    own_weight = own_weight * inverse
    parts = []
    for j in range(3):
        value = own_weight[:, j : j + 1] * value_own
        for k in range(Z):
            factor = factors[k] * inverse
            value = value + factor[:, j : j + 1] * rbuf[k, :, HD * j : HD * (j + 1)].astype(F32)
        parts.append(value)
    abuf[:, chip(z, CW)] = jnp.concatenate(parts, axis=1).astype(BF16)

    own_a = abuf.at[:, chip(z, CW)]
    a_sems = z_phase(lambda to: own_a, own_a, CW)
    w_d = []
    for d in range(1, X):
        w_x[d - 1].wait_recv()
        block = wbuf.at[c, (s + X - d) % X]
        w_d.append(remote(block, block, sem(), sem(), tp=partner))
        w_d[-1].start()
    local[2].wait()
    swaps[8].wait_recv()

    for copy in w_d:
        copy.wait_recv()
    all_a = block_wait(abuf.at[:, : (Z - 1) * CW], *a_sems)
    all_a.wait_recv()

    for k in range(2):
        part = jnp.zeros((8, D // (2 * Z)), F32)
        for e in range(X):
            part = part + lax.dot_general(
                abuf[:, DX * e : DX * (e + 1)], wbuf[k, e],
                (((1,), (1,)), ((), ())), preferred_element_type=F32,
            )
        pbuf[k, :, HD:] = jnp.zeros((8, HD), F32)
        pbuf[k, :, : D // (2 * Z)] = part
    both = [pbuf[k] for k in range(2)]
    resid = joined(tile(both[0], 0), tile(both[0], 1), tile(both[1], 0), tile(both[1], 1))
    resid = [a + b for a, b in zip(chip_tiles(hidden[half, :], phid[...]), resid)]
    resid = jnp.concatenate(resid, axis=1)
    gains = jnp.concatenate(chip_tiles(gain[...], pgain[...]), axis=1)[0:1]
    routers = jnp.concatenate(chip_tiles(router[...], prouter[...]), axis=1)
    gained = resid * gains
    hbuf[c, s, :, chip(z, CW)] = gained.astype(BF16)
    stats = jnp.where(lane == 0, jnp.sum(resid * resid, axis=1, keepdims=True), 0.0)
    for e in range(X):
        logit = jnp.sum(gained * routers[e : e + 1], axis=1, keepdims=True)
        stats = jnp.where(lane == e + 1, logit, stats)
    tbuf[z] = stats

    own_t, own_h = tbuf.at[z], hbuf.at[c, s, :, chip(z, CW)]
    t_sems = z_phase(lambda to: own_t, own_t, HD)
    h_sems = z_phase(lambda to: own_h, own_h, CW)
    all_t = block_wait(tbuf.at[: Z - 1], *t_sems)
    all_t.wait_recv()
    sums = tbuf[0]
    for k in range(1, Z):
        sums = sums + tbuf[k]
    inv_root = 1.0 / jnp.sqrt(sums[:, 0:1] / D + 1e-05)
    irb[c, s] = jnp.broadcast_to(inv_root, (8, HD))

    hx_sems = [[(sem(), sem()) for d in range(X)] for k in range(2)]
    hd_sems = [[(sem(), sem()) for d in range(X)] for k in range(2)]

    def h_x(k, d):
        ref = (hbuf, irb)[k]
        return remote(ref.at[c, s], ref.at[c, s], *hx_sems[k][d], sub=(s + d) % X)

    def h_d(k, d):
        ref = (hbuf, irb)[k].at[c, (s + X - d) % X]
        return remote(ref, ref, *hd_sems[k][d], tp=partner)

    for d in range(1, X):
        h_x(1, d).start()
    h_d(1, 0).start()
    logits = sums * inv_root
    hot_first, hot_second = lane == column(routes[0:1, :]) + 1, lane == column(routes[1:2, :]) + 1
    l_first = jnp.sum(jnp.where(hot_first, logits, 0.0), axis=1, keepdims=True)
    l_second = jnp.sum(jnp.where(hot_second, logits, 0.0), axis=1, keepdims=True)
    w_first = 1.0 / (1.0 + jnp.exp(l_second - l_first))
    w_second = 1.0 / (1.0 + jnp.exp(l_first - l_second))
    dense = jnp.where(hot_first, w_first, 0.0) + jnp.where(hot_second, w_second, 0.0)

    def share(e):
        return jnp.sum(jnp.where(lane == e + 1, dense, 0.0), axis=1, keepdims=True)

    all_h = block_wait(hbuf.at[c, s, :, : (Z - 1) * CW], *h_sems)
    all_h.wait_recv()
    for d in range(1, X):
        h_x(0, d).start()
    h_d(0, 0).start()
    for d in range(1, X):
        for k in (1, 0):
            h_x(k, d).wait_recv()
            h_d(k, d).start()
    for d in range(X):
        for k in (1, 0):
            h_d(k, d).wait_recv()
    for copy in local[3:]:
        copy.wait()

    N = 16 * X
    F = gbuf.shape[1]
    step = 6 * HD
    gate = jnp.zeros((N, F), F32)
    up = jnp.zeros((N, F), F32)
    for k in range(0, D, step):
        left = hbuf[:, :, :, k : k + step].astype(F32).reshape(N, step).astype(BF16)
        gate = gate + jnp.dot(left, gbuf[k : k + step], preferred_element_type=F32)
        up = up + jnp.dot(left, ubuf[k : k + step], preferred_element_type=F32)
    inv = irb[...].reshape(N, HD)
    inv = jnp.concatenate([inv] * (F // HD), axis=1)
    gate, up = gate * inv, up * inv
    inner[...] = (gate / (1.0 + jnp.exp(-gate)) * up).reshape(2, N // 2, F).astype(BF16)
    order = [0] * Z
    for k in range(Z - 1):
        order[k] = Z // 2 + (k // 2 if k % 2 == 0 else -((k + 1) // 2))
    per = Z // CHUNKS
    wide = per * CW
    targets = [(z + d) % Z for d in order]
    y_copies = []
    for h in range(CHUNKS):
        for p in range(per):
            at = slice(CW * p, CW * (p + 1))
            weight = dbuf[:, chip(targets[per * h + p], CW)]
            part = jnp.dot(inner[o], weight, preferred_element_type=F32)
            ysend[h, :, :, at] = part.reshape(X, 8, CW).astype(BF16)
        y_copies.append(remote(ysend.at[h], yrecv.at[h], sem(), sem(), tp=partner))
        y_copies[-1].start()
    for h in range(CHUNKS):
        for p in range(per):
            at = slice(CW * p, CW * (p + 1))
            weight = dbuf[:, chip(targets[per * h + p], CW)]
            part = jnp.dot(inner[c], weight, preferred_element_type=F32)
            ymine[h, :, :, at] = part.reshape(X, 8, CW)
    x_copies = []
    x_sems = [(sem(), sem()) for h in range(CHUNKS)]
    for h in range(CHUNKS):
        y_copies[h].wait_recv()
        for d in range(1, X):
            to = (s + d) % X
            xsend[h, d - 1] = (ymine[h, to] + yrecv[h, to].astype(F32)).astype(BF16)
            copy = remote(xsend.at[h, d - 1], xrecv.at[h, d - 1], *x_sems[h], sub=to)
            copy.start()
        x_copies.append(block_wait(xrecv.at[h], *x_sems[h]))
        acc[h] = share(s) * (ymine[h, s] + yrecv[h, s].astype(F32))
    z_sems = sem(), sem()
    for h in range(CHUNKS):
        x_copies[h].wait_recv()
        total = acc[h]
        for d in range(1, X):
            total = total + share((s + X - d) % X) * xrecv[h, d - 1].astype(F32)
        acc[h] = total
        zsend[h] = total.astype(BF16)
        for p in range(per):
            k = per * h + p
            if k < Z - 1:
                at = slice(CW * p, CW * (p + 1))
                remote(
                    zsend.at[h, :, at], zrecv.at[k], *z_sems, tp=2 * targets[k] + c
                ).start()
    result = resid + acc[CHUNKS - 1, :, (per - 1) * CW :]
    all_z = block_wait(zrecv, *z_sems)
    all_z.wait_recv()
    for k in range(Z - 1):
        result = result + zrecv[k].astype(F32)

    r1, r2 = pltpu.roll(tile(result, 1), 64, 1), pltpu.roll(tile(result, 2), 64, 1)
    v_first = result[:, : 2 * HD]
    v_second = jnp.concatenate([jnp.where(lane < 64, r1, r2), r2], axis=1)
    fsend[...] = pick(c, v_second, v_first).astype(BF16)
    f_copy = remote(fsend, frecv, sem(), sem(), tp=partner)
    f_copy.start()
    kept = pick(c, v_first, v_second)

    for copy in (all_q, all_o, all_a, all_h, all_t, all_z, kv_copy):
        copy.wait_send()
    for copy in swaps + w_x + w_d + y_copies + x_copies:
        copy.wait_send()
    for k in range(2):
        for d in range(1, X):
            h_x(k, d).wait_send()
        for d in range(X):
            h_d(k, d).wait_send()
    f_copy.wait()
    came = frecv[...].astype(F32)
    whole = jnp.concatenate([pick(c, kept, came), pick(c, came, kept)], axis=0)
    out[...] = whole[:, : D // (2 * Z)].astype(BF16)


def on_device(
    Z, X,
    hidden_in, query, key_new, value_new, key_cache, value_cache, lengths,
    out_weight, norm_gain, router_weight, routes, gate_weight, up_weight, down_weight,
):
    width = hidden_in.shape[1]
    D = width * 2 * Z
    P_LOC = key_cache.shape[1]
    F = gate_weight.shape[2]
    CW = 3 * HD
    KV = key_new.shape[1]
    W = D // CHUNKS
    vm = pl.BlockSpec(memory_space=pltpu.VMEM)
    anywhere = pl.BlockSpec(memory_space=pl.ANY)
    dma = pltpu.SemaphoreType.DMA
    V = pltpu.VMEM
    scratch = [
        V((8, width), BF16), V((8, width), BF16), V((8, KV), BF16), V((8, KV), BF16),
        V((1, width), BF16), V((X, width), BF16), V((4, 8, 2 * HD), F32),
        V((2, 8, P_LOC, key_cache.shape[2]), BF16), V((2, 8, P_LOC, key_cache.shape[2]), BF16),
        V((2, X, width, D // X), BF16),
        V((D, F), BF16), V((D, F), BF16), V((F, D), BF16),
        V((8, HD), BF16), V((8, HD), BF16),
        V((8, D), BF16),
        V((8, Z * 4 * HD), BF16), V((Z, 8, 4 * HD), BF16),
        V((8, D), BF16), V((2, 8, 2 * HD), F32),
        V((2, X, 8, D), BF16), V((Z, 8, HD), F32), V((2, X, 8, HD), F32),
        V((2, 8 * X, F), BF16),
        V((CHUNKS, X, 8, W), BF16), V((CHUNKS, X, 8, W), BF16), V((CHUNKS, X, 8, W), F32),
        V((CHUNKS, X - 1, 8, W), BF16), V((CHUNKS, X - 1, 8, W), BF16),
        V((CHUNKS, 8, W), F32), V((CHUNKS, 8, W), BF16), V((Z - 1, 8, CW), BF16),
        V((8, 2 * HD), BF16), V((8, 2 * HD), BF16),
        dma((6,)), dma((SEMAPHORES,)),
    ]
    return pl.pallas_call(
        functools.partial(layer, Z, X, D, P_LOC),
        out_shape=jax.ShapeDtypeStruct(hidden_in.shape, BF16),
        in_specs=[vm] * 8 + [anywhere] * 6,
        out_specs=vm,
        scratch_shapes=scratch,
        compiler_params=pltpu.CompilerParams(
            collective_id=0, has_side_effects=True, vmem_limit_bytes=56 * 1024 * 1024
        ),
        name="decode_layer",
    )(
        hidden_in, query, key_new, value_new, lengths[None], routes.T, norm_gain[None],
        router_weight.T, key_cache, value_cache, out_weight.T, gate_weight, up_weight, down_weight,
    )


def solution(mesh):
    Z, X = mesh.shape["tp"] // 2, mesh.shape["sub"]
    rows = P(("rep", "sub"), "tp")
    return jax.shard_map(
        functools.partial(on_device, Z, X),
        mesh=mesh,
        in_specs=(
            rows, rows, rows, rows,
            P(("rep", "sub"), "tp", None), P(("rep", "sub"), "tp", None), P(("rep", "sub")),
            P("sub", "tp"), P("tp"), P("tp", None), P(("rep", "sub"), None),
            P("sub", None, "tp"), P("sub", None, "tp"), P("sub", "tp", None),
        ),
        out_specs=rows,
        check_vma=False,
    )
```

```python
import functools

import jax
import jax.numpy as jnp
from jax import lax
from jax.experimental import pallas as pl
from jax.experimental.pallas import tpu as pltpu
from jax.sharding import PartitionSpec as P

HD = 128
F32 = jnp.float32
BF16 = jnp.bfloat16
MESH = pl.DeviceIdType.MESH
FLOOR = -1e30
CHUNKS = 4
SEMAPHORES = 112


def far_first(count):
    middle = count // 2
    far = [middle + (k // 2 if k % 2 == 0 else -((k + 1) // 2)) for k in range(count - 1)]
    return far + [0]


def lanes(shape):
    return lax.broadcasted_iota(jnp.int32, shape, len(shape) - 1)


def pick(flag, first, second):
    return jnp.where(jnp.full(first.shape, flag, jnp.int32) == 0, first, second)


def joined(a0, a1, b0, b1):
    lane = lanes(a0.shape)
    r0, r1 = pltpu.roll(b0, 64, 1), pltpu.roll(b1, 64, 1)
    return a0, jnp.where(lane < 64, a1, r0), jnp.where(lane < 64, r0, r1)


def layer(
    Z, X, D, P_LOC,
    hidden, query, k_new, v_new, lens, routes, gain, router, kc, vc, wo, gw, uw, dw,
    out,
    phid, pq, pk, pv, pgain, prouter, small,
    kbuf, vbuf, wbuf, gbuf, ubuf, dbuf,
    kvt, kvo, base, qbuf, obuf, rbuf, abuf, pbuf,
    hbuf, tbuf, irb, inner, ysend, yrecv, ymine, xsend, xrecv, acc, zsend, zrecv, fsend, frecv,
    lsem, sems, tokens,
):
    t = lax.axis_index("tp")
    s = lax.axis_index("sub")
    c = t % 2
    z = t // 2
    o = 1 - c
    partner = t + 1 - 2 * c
    CW = 3 * HD
    KVH = Z // 2
    DX = D // X
    taken = iter(range(SEMAPHORES))
    order = far_first(Z)
    targets = [(z + d) % Z for d in order]
    sources = [(z + Z - d) % Z for d in order]
    per = Z // CHUNKS
    scale = 1.0 / HD**0.5

    def sem():
        return sems.at[next(taken)]

    def remote(src, dst, ssem, rsem, **where):
        return pltpu.make_async_remote_copy(
            src_ref=src, dst_ref=dst, send_sem=ssem, recv_sem=rsem,
            device_id=where, device_id_type=MESH,
        )

    def over_z(fn):
        def step(k, carry):
            d = Z // 2 + jnp.where(k % 2 == 0, k // 2, -((k + 1) // 2))
            fn((z + d) % Z)
            return carry

        lax.fori_loop(0, Z - 1, step, 0)

    def z_phase(src, dst, width):
        ssem, rsem = sem(), sem()

        def send(to):
            remote(src(to), dst, ssem, rsem, tp=2 * to + c).start()

        over_z(send)
        return ssem, rsem

    def spread(ref):
        pairs = [(sem(), sem()) for h in range(CHUNKS)]
        for k in range(Z - 1):
            h, at = k // per, pl.ds(CW * (k % per), CW)
            remote(
                ref.at[CHUNKS - 1, :, (per - 1) * CW :], ref.at[h, :, at], *pairs[h],
                tp=2 * targets[k] + c,
            ).start()
        waits = [block_wait(ref.at[h], *pairs[h]) for h in range(CHUNKS - 1)]
        return waits + [block_wait(ref.at[CHUNKS - 1, :, : (per - 1) * CW], *pairs[-1])]

    def block_wait(ref, ssem, rsem):
        return remote(ref, ref, ssem, rsem, tp=partner)

    def chip(i, width):
        return pl.ds(pl.multiple_of(i * width, 128), width)

    half = pl.ds(pl.multiple_of(8 * c, 8), 8)
    other = pl.ds(pl.multiple_of(8 * o, 8), 8)
    local = [
        pltpu.make_async_copy(kc.at[half], kbuf.at[c], lsem.at[0]),
        pltpu.make_async_copy(vc.at[half], vbuf.at[c], lsem.at[1]),
        pltpu.make_async_copy(wo, wbuf.at[c, s], lsem.at[2]),
        pltpu.make_async_copy(gw.at[0], gbuf, lsem.at[3]),
        pltpu.make_async_copy(uw.at[0], ubuf, lsem.at[4]),
        pltpu.make_async_copy(dw.at[0], dbuf, lsem.at[5]),
    ]
    for copy in local:
        copy.start()

    barrier = pltpu.get_barrier_semaphore()

    def signal(what, **where):
        pl.semaphore_signal(what, inc=1, device_id=where, device_id_type=MESH)

    def around(d):
        return 2 * ((z + d) % Z) + c

    near = [d for k in range(Z // 4, 0, -1) for d in (k, -k)]
    for d in near:
        signal(barrier, tp=around(d))
    for d in range(1, X):
        signal(barrier, sub=(s + d) % X)
    signal(barrier, tp=partner)
    pl.semaphore_wait(barrier, len(near) + X - 1 + 1)

    def tell():
        signal(tokens.at[0], tp=around(Z // 4))
        signal(tokens.at[1], tp=around(-(Z // 4)))

    swaps = [
        remote(src, dst, sem(), sem(), tp=partner)
        for src, dst in (
            (query.at[other], pq), (k_new.at[other], pk), (v_new.at[other], pv),
            (hidden.at[other], phid), (gain, pgain), (router, prouter),
            (kc.at[other], kbuf.at[c]), (vc.at[other], vbuf.at[c]), (wo, wbuf.at[c, s]),
        )
    ]
    for copy in swaps:
        copy.start()
    ways = (1, X - 1) if X == 4 else range(1, X)
    w_x = {
        d: remote(wo, wbuf.at[c, s], sem(), sem(), sub=(s + d) % X) for d in ways
    }
    for copy in w_x.values():
        copy.start()
    tell()
    lane = lanes((8, HD))

    def tile(value, k):
        return value[:, HD * k : HD * (k + 1)]

    def widened(*parts):
        pairs = []
        for k, part in enumerate(parts):
            small[k, : part.shape[0], : part.shape[1]] = part.astype(F32)
            pairs.append((small[k, :, :HD], small[k, :, HD:]))
        return pairs

    def chip_tiles(own, came):
        (o0, o1), (c0, c1) = widened(own, came)
        return joined(pick(c, o0, c0), pick(c, o1, c1), pick(c, c0, o0), pick(c, c1, o1))

    small[...] = jnp.zeros(small.shape, F32)
    swaps[0].wait_recv()

    q_own = chip_tiles(query[half, :], pq[...])
    qbuf[:, chip(z, CW)] = jnp.concatenate(q_own, axis=1).astype(BF16)

    own_q = qbuf.at[:, chip(z, CW)]
    bands = Z // 4 + 1
    q_sems = [(sem(), sem()) for b in range(bands)]
    pl.semaphore_wait(tokens.at[0], 1)
    pl.semaphore_wait(tokens.at[1], 1)
    for d in order[:-1]:
        band = min(d, Z - d) // 2
        remote(own_q, own_q, *q_sems[band], tp=around(d)).start()
    sizes = [sum(min(d, Z - d) // 2 == b for d in range(1, Z)) for b in range(bands)]
    q_waits = [block_wait(qbuf.at[:, : n * CW], *q_sems[b]) for b, n in enumerate(sizes)]
    for copy in swaps[1:6]:
        copy.wait_recv()
    small[...] = jnp.zeros(small.shape, F32)
    kv = [v[0] for v in widened(k_new[half, :], v_new[half, :], pk[...], pv[...])]
    kv = [pick(c, kv[0], kv[2]), pick(c, kv[1], kv[3]), pick(c, kv[2], kv[0]), pick(c, kv[3], kv[1])]
    kv = [kv[0]] + [pltpu.roll(v, 32 * (k + 1), 1) for k, v in enumerate(kv[1:])]
    kvt[...] = (kv[0] + kv[1] + kv[2] + kv[3]).astype(BF16)
    z_pair = z + 1 - 2 * (z % 2)
    kv_copy = remote(kvt, kvo, sem(), sem(), tp=2 * z_pair + c)
    kv_copy.start()

    base[0] = jnp.concatenate(chip_tiles(hidden[half, :], phid[...]), axis=1)
    base[1] = jnp.concatenate(chip_tiles(gain[...].reshape(1, -1), pgain[...].reshape(1, -1)), axis=1)
    base[2] = jnp.concatenate(chip_tiles(router[...], prouter[...]), axis=1)
    local[0].wait()
    local[1].wait()
    swaps[6].wait_recv()
    swaps[7].wait_recv()

    cols = 2 * 8 * P_LOC
    group = 6
    rows = group * 8
    col = lax.broadcasted_iota(jnp.int32, (rows, cols), 1)
    row = lax.broadcasted_iota(jnp.int32, (rows, cols), 0)
    position = (2 * z + col // (8 * P_LOC)) * P_LOC + col % P_LOC
    slot = lax.broadcasted_iota(jnp.int32, (8, 16), 1)
    chosen = slot == lax.broadcasted_iota(jnp.int32, (8, 16), 0) + 8 * c

    def column(line):
        picked = jnp.where(chosen, jnp.broadcast_to(line.astype(F32), (8, 16)), 0.0)
        return jnp.sum(picked, axis=1, keepdims=True).astype(jnp.int32)

    length = jnp.broadcast_to(column(lens[...]), (8, cols))
    length = jnp.concatenate([length] * group, axis=0)
    valid = (row % 8 == (col % (8 * P_LOC)) // P_LOC) & (position < length)
    o_sems = sem(), sem()

    def send_o(to):
        remote(obuf.at[:, chip(to, 4 * HD)], rbuf.at[z], *o_sems, tp=2 * to + c).start()

    ready = []
    for turn in far_first(KVH)[::-1]:
        band = min(turn, KVH - turn)
        if band not in ready:
            q_waits[band].wait_recv()
            ready.append(band)
        g = (z // 2 + turn) % KVH
        at = chip(g, HD)
        q_g = qbuf[:, chip(g, group * HD)].astype(F32)
        q_g = jnp.concatenate([tile(q_g, i) for i in range(group)], axis=0).astype(BF16)
        keys = kbuf[:, :, :, at].reshape(cols, HD)
        values = vbuf[:, :, :, at].reshape(cols, HD)
        scores = (
            lax.dot_general(q_g, keys, (((1,), (1,)), ((), ())), preferred_element_type=F32) * scale
        )
        scores = jnp.where(valid, scores, FLOOR)
        top = jnp.max(scores, axis=1, keepdims=True).astype(BF16).astype(F32)
        weights = jnp.where(valid, jnp.exp(scores - top), 0.0)
        total = jnp.sum(weights, axis=1, keepdims=True)
        summed = jnp.dot(weights.astype(BF16), values, preferred_element_type=F32)
        high = total.astype(BF16).astype(F32)
        low = total - high
        for k in range(2):
            stats = jnp.zeros((8, HD), F32)
            parts = []
            for j in range(3):
                at_row = slice(8 * (3 * k + j), 8 * (3 * k + j + 1))
                parts.append(summed[at_row])
                stats = jnp.where(lane == j, top[at_row], stats)
                stats = jnp.where(lane == 32 + j, high[at_row], stats)
                stats = jnp.where(lane == 64 + j, low[at_row], stats)
            block = jnp.concatenate(parts + [stats], axis=1).astype(BF16)
            obuf[:, chip(2 * g + k, 4 * HD)] = block
        if turn:
            send_o(2 * g)
            send_o(2 * g + 1)
        else:
            send_o(z_pair)
    w_d, w_r = [], []
    top_half = wbuf.shape[2] // 2

    def handed_on(ref):
        copy = remote(ref, ref, sem(), sem(), tp=partner)
        copy.start()
        return copy

    for d, copy in w_x.items():
        copy.wait_recv()
        block = wbuf.at[c, (s + X - d) % X]
        if X == 4:
            part = block.at[pl.ds(0 if d == 1 else top_half, top_half)]
            w_r.append(remote(part, part, sem(), sem(), sub=(s + d) % X))
            w_r[-1].start()
        w_d.append(handed_on(block))
    rbuf[z] = obuf[:, chip(z, 4 * HD)]
    kv_copy.wait_recv()
    t_mine, t_pair = kvt[...].astype(F32), kvo[...].astype(F32)
    even, odd = pick(z % 2, t_mine, t_pair), pick(z % 2, t_pair, t_mine)

    def quarters(shifts):
        w = [pltpu.roll(v, k, 1) if k else v for v, k in zip((even, even, odd, odd), shifts)]
        low_half = jnp.where(lane < 32, w[0], w[1])
        high_half = jnp.where(lane < 96, w[2], w[3])
        return jnp.where(lane < 64, low_half, high_half)

    key_own = quarters((0, 96, 64, 32))
    value_own = quarters((96, 64, 32, 0))
    own = jnp.zeros((8, HD), F32)
    for j in range(3):
        dot = jnp.sum(q_own[j] * key_own, axis=1, keepdims=True) * scale
        own = jnp.where(lane == j, dot, own)

    all_o = block_wait(rbuf.at[: Z - 1], *o_sems)
    all_o.wait_recv()
    tops = [rbuf[k, :, 3 * HD :].astype(F32) for k in range(Z)]
    top = own
    for part in tops:
        top = jnp.maximum(top, part)
    own_weight = jnp.where(lane < 3, jnp.exp(own - top), 0.0)
    total = own_weight
    factors = []
    for part in tops:
        factor = jnp.where(lane < 3, jnp.exp(part - top), 0.0)
        factors.append(factor)
        total = total + factor * (pltpu.roll(part, 96, 1) + pltpu.roll(part, 64, 1))
    inverse = jnp.where(lane < 3, 1.0 / jnp.where(lane < 3, total, 1.0), 0.0)
    own_weight = own_weight * inverse
    parts = []
    for j in range(3):
        value = own_weight[:, j : j + 1] * value_own
        for k in range(Z):
            factor = factors[k] * inverse
            value = value + factor[:, j : j + 1] * rbuf[k, :, HD * j : HD * (j + 1)].astype(F32)
        parts.append(value)
    abuf[CHUNKS - 1, :, (per - 1) * CW :] = jnp.concatenate(parts, axis=1).astype(BF16)
    a_waits = spread(abuf)
    if X == 4:
        block = wbuf.at[c, (s + 2) % X]
        for copy in w_r:
            copy.wait_recv()
        w_d.append(handed_on(block))
    local[2].wait()
    swaps[8].wait_recv()

    for copy in w_d:
        copy.wait_recv()
    sums = [jnp.zeros((8, D // (2 * Z)), F32) for k in range(2)]
    for h in reversed(range(CHUNKS)):
        a_waits[h].wait_recv()
        for p in range(per):
            source = sources[per * h + p]
            e, at = source // (Z // X), chip(source % (Z // X), CW)
            for k in range(2):
                sums[k] = sums[k] + lax.dot_general(
                    abuf[h, :, CW * p : CW * (p + 1)], wbuf[k, e, :, at],
                    (((1,), (1,)), ((), ())), preferred_element_type=F32,
                )
    for k in range(2):
        pbuf[k, :, HD:] = jnp.zeros((8, HD), F32)
        pbuf[k, :, : D // (2 * Z)] = sums[k]
    both = [pbuf[k] for k in range(2)]
    resid = joined(tile(both[0], 0), tile(both[0], 1), tile(both[1], 0), tile(both[1], 1))
    resid = base[0] + jnp.concatenate(resid, axis=1)
    gains, routers = base[1, 0:1], base[2]
    gained = resid * gains
    stats = jnp.where(lane == 0, jnp.sum(resid * resid, axis=1, keepdims=True), 0.0)
    for e in range(X):
        logit = jnp.sum(gained * routers[e : e + 1], axis=1, keepdims=True)
        stats = jnp.where(lane == e + 1, logit, stats)
    high = stats.astype(BF16).astype(F32)
    middle = (stats - high).astype(BF16).astype(F32)
    low = stats - high - middle
    tbuf[z] = (high + pltpu.roll(middle, 32, 1) + pltpu.roll(low, 64, 1)).astype(BF16)
    own_t = tbuf.at[z]
    t_sems = z_phase(lambda to: own_t, own_t, HD)
    own_h = hbuf.at[c, :, 0]
    own_h[CHUNKS - 1, :, (per - 1) * CW :] = gained.astype(BF16)
    h_waits = spread(own_h)
    hx_sems = [(sem(), sem()) for h in range(CHUNKS)]
    x_waits = [block_wait(hbuf.at[c, h, 1:], *hx_sems[h]) for h in range(CHUNKS)]
    for h in reversed(range(CHUNKS)):
        h_waits[h].wait_recv()
        for d in range(1, X):
            remote(hbuf.at[c, h, 0], hbuf.at[c, h, d], *hx_sems[h], sub=(s + d) % X).start()
    all_t = block_wait(tbuf.at[: Z - 1], *t_sems)
    all_t.wait_recv()
    sums = tbuf[0].astype(F32)
    for k in range(1, Z):
        sums = sums + tbuf[k].astype(F32)
    sums = sums + pltpu.roll(sums, 96, 1) + pltpu.roll(sums, 64, 1)
    inv_root = 1.0 / jnp.sqrt(sums[:, 0:1] / D + 1e-05)
    irb[c, 0] = jnp.broadcast_to(inv_root, (8, HD))
    ix_sems = sem(), sem()
    for d in range(1, X):
        remote(irb.at[c, 0], irb.at[c, d], *ix_sems, sub=(s + d) % X).start()
    ix_wait = block_wait(irb.at[c, 1:], *ix_sems)
    logits = sums * inv_root
    hot_first, hot_second = lane == column(routes[0:1, :]) + 1, lane == column(routes[1:2, :]) + 1
    l_first = jnp.sum(jnp.where(hot_first, logits, 0.0), axis=1, keepdims=True)
    l_second = jnp.sum(jnp.where(hot_second, logits, 0.0), axis=1, keepdims=True)
    w_first = 1.0 / (1.0 + jnp.exp(l_second - l_first))
    w_second = 1.0 / (1.0 + jnp.exp(l_first - l_second))
    dense = jnp.where(hot_first, w_first, 0.0) + jnp.where(hot_second, w_second, 0.0)

    def share(e):
        return jnp.sum(jnp.where(lane == e + 1, dense, 0.0), axis=1, keepdims=True)

    N = 16 * X
    F = gbuf.shape[1]
    for copy in local[3:]:
        copy.wait()
    gate = jnp.zeros((N, F), F32)
    up = jnp.zeros((N, F), F32)
    d_copies = {}

    def columns(h, gate, up):
        d_copies[h].wait_recv()
        rows_in = hbuf[:, h].astype(F32).reshape(N, per * CW).astype(BF16)
        for p in range(per):
            left = rows_in[:, CW * p : CW * (p + 1)]
            at = chip(sources[per * h + p], CW)
            gate = gate + jnp.dot(left, gbuf[at, :], preferred_element_type=F32)
            up = up + jnp.dot(left, ubuf[at, :], preferred_element_type=F32)
        return gate, up

    for h in reversed(range(CHUNKS)):
        x_waits[h].wait_recv()
        d_copies[h] = handed_on(hbuf.at[c, h])
        if h == 0:
            ix_wait.wait_recv()
            i_copy = handed_on(irb.at[c])
        if h + 1 < CHUNKS:
            gate, up = columns(h + 1, gate, up)
    gate, up = columns(0, gate, up)
    i_copy.wait_recv()
    inv = irb[...].reshape(N, HD)
    inv = jnp.concatenate([inv] * (F // HD), axis=1)
    gate, up = gate * inv, up * inv
    inner[...] = (gate / (1.0 + jnp.exp(-gate)) * up).reshape(2, N // 2, F).astype(BF16)
    y_copies = []
    for h in range(CHUNKS):
        for p in range(per):
            at = slice(CW * p, CW * (p + 1))
            weight = dbuf[:, chip(targets[per * h + p], CW)]
            part = jnp.dot(inner[o], weight, preferred_element_type=F32)
            ysend[h, :, :, at] = part.reshape(X, 8, CW).astype(BF16)
        y_copies.append(remote(ysend.at[h], yrecv.at[h], sem(), sem(), tp=partner))
        y_copies[-1].start()
    x_copies = []
    x_sems = [(sem(), sem()) for h in range(CHUNKS)]
    for h in range(CHUNKS):
        for p in range(per):
            at = slice(CW * p, CW * (p + 1))
            weight = dbuf[:, chip(targets[per * h + p], CW)]
            part = jnp.dot(inner[c], weight, preferred_element_type=F32)
            ymine[h, :, :, at] = part.reshape(X, 8, CW)
        y_copies[h].wait_recv()
        for d in range(1, X):
            to = (s + X - d) % X
            xsend[h, d - 1] = (ymine[h, d] + yrecv[h, d].astype(F32)).astype(BF16)
            copy = remote(xsend.at[h, d - 1], xrecv.at[h, d - 1], *x_sems[h], sub=to)
            copy.start()
        x_copies.append(block_wait(xrecv.at[h], *x_sems[h]))
        acc[h] = share(s) * (ymine[h, 0] + yrecv[h, 0].astype(F32))
    z_sems = sem(), sem()
    for h in range(CHUNKS):
        x_copies[h].wait_recv()
        total = acc[h]
        for d in range(1, X):
            total = total + share((s + d) % X) * xrecv[h, d - 1].astype(F32)
        acc[h] = total
        zsend[h] = total.astype(BF16)
        for p in range(per):
            k = per * h + p
            if k < Z - 1:
                at = slice(CW * p, CW * (p + 1))
                remote(
                    zsend.at[h, :, at], zrecv.at[k], *z_sems, tp=2 * targets[k] + c
                ).start()
    result = resid + acc[CHUNKS - 1, :, (per - 1) * CW :]
    all_z = block_wait(zrecv, *z_sems)
    all_z.wait_recv()
    for k in range(Z - 1):
        result = result + zrecv[k].astype(F32)

    r1, r2 = pltpu.roll(tile(result, 1), 64, 1), pltpu.roll(tile(result, 2), 64, 1)
    v_first = result[:, : 2 * HD]
    v_second = jnp.concatenate([jnp.where(lane < 64, r1, r2), r2], axis=1)
    fsend[...] = pick(c, v_second, v_first).astype(BF16)
    f_copy = remote(fsend, frecv, sem(), sem(), tp=partner)
    f_copy.start()
    kept = pick(c, v_first, v_second)

    for copy in [all_o, all_t, all_z, kv_copy, ix_wait, i_copy] + a_waits + h_waits + q_waits:
        copy.wait_send()
    for copy in swaps + list(w_x.values()) + w_r + w_d + y_copies + x_copies + x_waits + list(d_copies.values()):
        copy.wait_send()
    f_copy.wait()
    came = frecv[...].astype(F32)
    whole = jnp.concatenate([pick(c, kept, came), pick(c, came, kept)], axis=0)
    out[...] = whole[:, : D // (2 * Z)].astype(BF16)


def on_device(
    Z, X,
    hidden_in, query, key_new, value_new, key_cache, value_cache, lengths,
    out_weight, norm_gain, router_weight, routes, gate_weight, up_weight, down_weight,
):
    width = hidden_in.shape[1]
    D = width * 2 * Z
    P_LOC = key_cache.shape[1]
    F = gate_weight.shape[2]
    CW = 3 * HD
    KV = key_new.shape[1]
    W = D // CHUNKS
    vm = pl.BlockSpec(memory_space=pltpu.VMEM)
    anywhere = pl.BlockSpec(memory_space=pl.ANY)
    dma = pltpu.SemaphoreType.DMA
    V = pltpu.VMEM
    scratch = [
        V((8, width), BF16), V((8, width), BF16), V((8, KV), BF16), V((8, KV), BF16),
        V((width,), BF16), V((X, width), BF16), V((4, 8, 2 * HD), F32),
        V((2, 8, P_LOC, key_cache.shape[2]), BF16), V((2, 8, P_LOC, key_cache.shape[2]), BF16),
        V((2, X, width, D // X), BF16),
        V((D, F), BF16), V((D, F), BF16), V((F, D), BF16),
        V((8, HD), BF16), V((8, HD), BF16), V((3, 8, CW), F32),
        V((8, D), BF16),
        V((8, Z * 4 * HD), BF16), V((Z, 8, 4 * HD), BF16),
        V((CHUNKS, 8, W), BF16), V((2, 8, 2 * HD), F32),
        V((2, CHUNKS, X, 8, W), BF16), V((Z, 8, HD), BF16), V((2, X, 8, HD), F32),
        V((2, 8 * X, F), BF16),
        V((CHUNKS, X, 8, W), BF16), V((CHUNKS, X, 8, W), BF16), V((CHUNKS, X, 8, W), F32),
        V((CHUNKS, X - 1, 8, W), BF16), V((CHUNKS, X - 1, 8, W), BF16),
        V((CHUNKS, 8, W), F32), V((CHUNKS, 8, W), BF16), V((Z - 1, 8, CW), BF16),
        V((8, 2 * HD), BF16), V((8, 2 * HD), BF16),
        dma((6,)), dma((SEMAPHORES,)), pltpu.SemaphoreType.REGULAR((2,)),
    ]
    return pl.pallas_call(
        functools.partial(layer, Z, X, D, P_LOC),
        out_shape=jax.ShapeDtypeStruct(hidden_in.shape, BF16),
        in_specs=[vm] * 8 + [anywhere] * 6,
        out_specs=vm,
        scratch_shapes=scratch,
        compiler_params=pltpu.CompilerParams(
            collective_id=0, has_side_effects=True, vmem_limit_bytes=56 * 1024 * 1024
        ),
        name="decode_layer",
    )(
        hidden_in, query, key_new, value_new, lengths[None], routes.T, norm_gain,
        router_weight.T, key_cache, value_cache, out_weight.T, gate_weight, up_weight, down_weight,
    )


def solution(mesh):
    Z, X = mesh.shape["tp"] // 2, mesh.shape["sub"]
    rows = P(("rep", "sub"), "tp")
    return jax.shard_map(
        functools.partial(on_device, Z, X),
        mesh=mesh,
        in_specs=(
            rows, rows, rows, rows,
            P(("rep", "sub"), "tp", None), P(("rep", "sub"), "tp", None), P(("rep", "sub")),
            P("sub", "tp"), P("tp"), P("tp", None), P(("rep", "sub"), None),
            P("sub", None, "tp"), P("sub", None, "tp"), P("sub", "tp", None),
        ),
        out_specs=rows,
        check_vma=False,
    )
```
